32 devices in a mesh: col: 16 (over z, x, core), row: 2 (over y).
Axes of the slice: x: 2, y: 2, z: 4, core: 2. Of those that a mesh axis runs over, the one named last changes fastest.
Arguments:
- blocks: float32 [16, 2, 24, 128, 128], P('col', 'row'), may hold values from -0.21875 to 0.21875
- row_index: int32 [16, 2, 24], P('col', 'row'), may hold values from 0 to 63
- col_index: int32 [16, 2, 24], P('col', 'row'), may hold values from 0 to 23
- counts: int32 [16, 2], P('col', 'row'), may hold values from 12 to 24, as said below
- rhs: float32 [16384], P(('row', 'col')), may hold values from -6 to 6
- lower: float32 [49152], P(('col', 'row')), may hold values from -0.6 to -0.05
- upper: float32 [49152], P(('col', 'row')), may hold values from 0.05 to 0.6
- primal_start: float32 [49152], P(('col', 'row')), may hold values from -0.05 to 0.05
- dual_start: float32 [16384], P(('row', 'col')), may hold values from -4 to 4
Outputs:
- primal: float32 [49152], P(('col', 'row'))
- dual: float32 [16384], P(('row', 'col'))
- norms: float32 [3, 2], replicated
The draws below stay inside these ranges and needn't reach their ends.
Inputs may be any that keep to these rules, and one draw needn't show every extreme that they name: `counts`: each list has between 12 and 24 live slots; both ends are reached in every draw.
All inputs are finite; a program needn't handle non-finite values.
Results may differ from the reference program's by a relative error of at most 0.0001.
Values sent between devices are 32-bit elements; how exact they have to be, the bound alone decides.
A program may use at most 64 MiB of HBM per device.

```python
import jax
import jax.numpy as jnp
from jax import lax

B = 128
KB = 24
RB_DEV = 4
ITERS = 3
CBG = 24
RBG = 64
NV = 49152
NC = 16384
N_COL = 16
N_ROW = 2


def draw_counts(key, part):
    first, second, third = jax.random.split(key, 3)
    total = N_COL * N_ROW
    values = jax.random.randint(first, (total,), KB // 2, KB + 1)
    where_top = jax.random.randint(second, (), 0, total)
    values = values.at[where_top].set(KB)
    where_low = (where_top + 1 + jax.random.randint(third, (), 0, total - 1)) % total
    values = values.at[where_low].set(KB // 2)
    return values.reshape(N_COL, N_ROW).astype(jnp.int32)


def with_ends(array, stream_key, least, largest):
    place = [jax.random.randint(jax.random.fold_in(stream_key, axis), (), 0, length) for axis, length in enumerate(array.shape)]
    main_axis = array.shape.index(max(array.shape))
    neighbour = place[:main_axis] + [(place[main_axis] + 1) % array.shape[main_axis]] + place[main_axis + 1:]
    return array.at[tuple(place)].set(least).at[tuple(neighbour)].set(largest)


def shard_levels(rng, extent, cuts, low, top_value):
    factor_of, own = 1.0, jax.random.fold_in(rng, 6)
    for axis_at, blocks in cuts:
        steps = jnp.exp(jax.random.uniform(jax.random.fold_in(own, axis_at), (blocks,), jnp.float32, low / len(cuts), top_value / len(cuts)))
        factor_of = factor_of * jnp.repeat(steps, extent[axis_at] // blocks).reshape([-1 if axis == axis_at else 1 for axis in range(len(extent))])
    return factor_of


def scatter_about(stream_key, extent, scale, limit, shards=(), kind=jnp.bfloat16):
    loudness = shard_levels(stream_key, extent, shards, -0.22, 0.18) if shards else 1.0
    entries = jax.random.normal(stream_key, extent, jnp.float32) * scale * loudness
    return jnp.minimum(jnp.maximum(entries, -limit), limit).astype(kind)


def setup_inputs(seed: int = 0) -> dict:
    key_of = jax.random.split(jax.random.key(seed), 10)
    blocks = scatter_about(key_of[0], (N_COL, N_ROW, KB, B, B), (KB * B // RB_DEV) ** -0.5, 0.21875, ((0, 16), (1, 2)), jnp.float32)
    row_index = with_ends(jax.random.randint(key_of[1], (N_COL, N_ROW, KB), 0, RBG), jax.random.fold_in(key_of[1], 1), 0, RBG - 1).astype(jnp.int32)
    col_index = with_ends(jax.random.randint(key_of[2], (N_COL, N_ROW, KB), 0, CBG), jax.random.fold_in(key_of[2], 1), 0, CBG - 1).astype(jnp.int32)
    counts = draw_counts(jax.random.fold_in(key_of[9], 71), 0)
    rhs = scatter_about(key_of[4], (NC,), 1.0, 6.0, ((0, 32),), jnp.float32)
    lower = jnp.clip(-0.6 + 0.55 * jax.random.uniform(key_of[5], (NV,), jnp.float32) ** shard_levels(key_of[5], (NV,), ((0, 32),), -0.2, 0.2), -0.6, -0.05)
    upper = jnp.clip(0.05 + 0.55 * jax.random.uniform(key_of[6], (NV,), jnp.float32) ** shard_levels(key_of[6], (NV,), ((0, 32),), -0.2, 0.2), 0.05, 0.6)
    primal_start = jnp.clip(jax.random.uniform(key_of[7], (NV,), jnp.float32, -0.05, 0.05) * shard_levels(key_of[7], (NV,), ((0, 32),), -0.4, 0.0), -0.05, 0.05)
    dual_start = scatter_about(key_of[8], (NC,), 0.5, 4.0, ((0, 32),), jnp.float32)
    return dict(blocks=blocks, row_index=row_index, col_index=col_index, counts=counts, rhs=rhs, lower=lower, upper=upper, primal_start=primal_start, dual_start=dual_start)


def reference(blocks, row_index, col_index, counts, rhs, lower, upper, primal_start, dual_start):
    tiles = blocks.reshape(-1, B, B)
    col_base = (jnp.arange(N_COL, dtype=jnp.int32) * CBG).reshape(N_COL, 1, 1)
    row_base = (jnp.arange(N_ROW, dtype=jnp.int32) * RBG).reshape(1, N_ROW, 1)
    global_rows = (row_index + row_base).reshape(-1).astype(jnp.int32)
    global_cols = (col_index + col_base).reshape(-1).astype(jnp.int32)
    slots = jnp.arange(KB, dtype=jnp.int32).reshape(1, 1, KB)
    live = (slots < counts[:, :, None]).astype(jnp.float32).reshape(-1)
    tau = 0.4
    sigma = 0.4

    def apply(vector):
        pieces = vector.reshape(-1, B)[global_cols]
        prod = jnp.einsum('kij,kj->ki', tiles, pieces, precision=lax.Precision.HIGHEST) * live[:, None]
        return jax.ops.segment_sum(prod, global_rows, num_segments=NC // B).reshape(-1)

    def transpose_apply(vector):
        pieces = vector.reshape(-1, B)[global_rows]
        prod = jnp.einsum('kij,ki->kj', tiles, pieces, precision=lax.Precision.HIGHEST) * live[:, None]
        return jax.ops.segment_sum(prod, global_cols, num_segments=NV // B).reshape(-1)
    primal = primal_start
    dual = dual_start
    records = []
    for step in range(ITERS):
        grad = transpose_apply(dual)
        primal_new = jnp.minimum(jnp.maximum(primal + tau * grad, lower), upper)
        extra = 2.0 * primal_new - primal
        resid = rhs - apply(extra)
        dual = dual + sigma * resid
        moved = primal_new - primal
        records.append(jnp.stack([jnp.sqrt(jnp.sum(resid * resid)), jnp.sqrt(jnp.sum(moved * moved))]))
        primal = primal_new
    return (primal, dual, jnp.stack(records))
```

```python
import functools

import jax
import jax.numpy as jnp
from jax import lax
from jax.experimental import pallas as pl
from jax.experimental.pallas import tpu as pltpu
from jax.sharding import PartitionSpec as P

ITERS = 3
TAU = 0.4
SIGMA = 0.4
MESH = pl.DeviceIdType.MESH


def each(count, body):
    if count <= 32:
        for step in range(1, count):
            body(step)
    else:
        lax.fori_loop(1, count, lambda step, carry: (body(step), carry)[1], 0)


def split(value):
    high = value.astype(jnp.bfloat16).astype(jnp.float32)
    return high, value - high


def left_operand(value):
    high, low = split(value)
    first = jnp.concatenate([high, low], axis=0)
    second = jnp.concatenate([high, jnp.zeros_like(low)], axis=0)
    return jnp.concatenate([first, second], axis=1).astype(jnp.bfloat16)


def kernel(
    n_col, n_row,
    blocks, rows, cols, counts, rhs, lower, upper, primal, dual,
    primal_out, dual_out, norms_out,
    tiles, w_t, w_n, pieces,
    bounds, own_vec, y_buf, g_buf, p_send, p_recv, x_ref, z_ref, n_buf,
    load_sem, own_sem, bound_send, bound_recv, y_send_sem, y_recv_sem,
    g_send_sem, g_recv_sem, p_send_sem, p_recv_sem, n_send_sem, n_recv_sem,
):
    slots, side = tiles.shape[0], tiles.shape[1]
    dual_rows = dual.shape[0]
    primal_rows = primal.shape[0]
    row_blocks = dual_rows * n_col
    col_blocks = primal_rows * n_row
    total = n_col * n_row
    me_col = lax.axis_index("col")
    me_row = lax.axis_index("row")
    me = me_col * n_row + me_row

    load = pltpu.make_async_copy(blocks, tiles, load_sem)
    load.start()
    own_copies = []
    for index, source in enumerate((primal, lower, upper)):
        copy = pltpu.make_async_copy(source, bounds.at[index, me_row], own_sem.at[index])
        copy.start()
        own_copies.append(copy)
    for index, (source, target) in enumerate(((dual, y_buf.at[0, me_col]), (rhs, own_vec))):
        copy = pltpu.make_async_copy(source, target, own_sem.at[3 + index])
        copy.start()
        own_copies.append(copy)

    barrier = pltpu.get_barrier_semaphore()

    def greet(step):
        other = lax.rem(me + step, total)
        pl.semaphore_signal(
            barrier, inc=1, device_id=(other // n_row, lax.rem(other, n_row)), device_id_type=MESH
        )

    each(total, greet)
    pl.semaphore_wait(barrier, total - 1)

    def to_col(source, target, send, recv):
        def body(step):
            other = lax.rem(me_col + step, n_col)
            pltpu.make_async_remote_copy(
                src_ref=source(other), dst_ref=target, send_sem=send, recv_sem=recv,
                device_id=(other, me_row), device_id_type=MESH,
            ).start()

        each(n_col, body)

    def to_row(source, target, send, recv):
        def body(step):
            other = lax.rem(me_row + step, n_row)
            pltpu.make_async_remote_copy(
                src_ref=source, dst_ref=target, send_sem=send, recv_sem=recv,
                device_id=(me_col, other), device_id_type=MESH,
            ).start()

        each(n_row, body)

    def await_bytes(ref, sem):
        pltpu.make_async_copy(ref, ref, sem).wait()

    to_col(lambda other: dual, y_buf.at[0, me_col], y_send_sem.at[0], y_recv_sem.at[0])
    for index, source in enumerate((primal, lower, upper)):
        to_row(source, bounds.at[index, me_row], bound_send.at[index], bound_recv.at[index])

    load.wait()
    for k in range(slots):
        tile = tiles[k]
        high, low = split(tile)
        w_t[0:side, k * side : (k + 1) * side] = high.astype(jnp.bfloat16)
        w_t[side : 2 * side, k * side : (k + 1) * side] = low.astype(jnp.bfloat16)
        high, low = split(tile.T)
        w_n[0:side, k * side : (k + 1) * side] = high.astype(jnp.bfloat16)
        w_n[side : 2 * side, k * side : (k + 1) * side] = low.astype(jnp.bfloat16)

    live = counts[0, 0]
    row_of = [rows[0, k] for k in range(slots)]
    col_of = [cols[0, k] for k in range(slots)]
    row_to = [jnp.where(k < live, row_of[k], -1) for k in range(slots)]
    col_to = [jnp.where(k < live, col_of[k], -1) for k in range(slots)]

    def products(weights):
        left = left_operand(pieces[...])
        outs = []
        group = 4
        for base in range(0, slots, group):
            end = min(slots, base + group)
            result = jnp.dot(
                left, weights[:, base * side : end * side], preferred_element_type=jnp.float32
            )
            for k in range(base, end):
                at = slice((k - base) * side, (k - base + 1) * side)
                outs.append(result[k : k + 1, at] + result[slots + k : slots + k + 1, at])
        return outs

    def spread(outs, targets, count):
        places = lax.broadcasted_iota(jnp.int32, (count, side), 0)
        total_value = jnp.zeros((count, side), jnp.float32)
        for k in range(slots):
            total_value += jnp.where(places == targets[k], outs[k], 0.0)
        return total_value

    for copy in own_copies:
        copy.wait()
    for index in range(3):
        await_bytes(bounds.at[index, pl.ds(0, n_row - 1)], bound_recv.at[index])
    groups = []
    for index in range(3):
        groups.append(jnp.concatenate([bounds[index, r] for r in range(n_row)], axis=0))
    x_value, low_value, high_value = groups
    x_ref[0] = x_value
    x_ref[1] = low_value
    x_ref[2] = high_value
    y_own = y_buf[0, me_col]
    rhs_own = own_vec[...]
    owner = lax.broadcasted_iota(jnp.int32, (col_blocks, side), 0) // primal_rows
    sums = []

    for step in range(ITERS):
        await_bytes(y_buf.at[step, pl.ds(0, n_col - 1)], y_recv_sem.at[step])
        for k in range(slots):
            r = row_of[k]
            pieces[k : k + 1, :] = y_buf[step, r // dual_rows, pl.ds(lax.rem(r, dual_rows), 1), :]
        partial = spread(products(w_t), col_to, col_blocks)
        g_buf[step, me_row] = partial
        to_row(
            g_buf.at[step, me_row], g_buf.at[step, me_row], g_send_sem.at[step], g_recv_sem.at[step]
        )
        await_bytes(g_buf.at[step, pl.ds(0, n_row - 1)], g_recv_sem.at[step])
        grad = g_buf[step, 0]
        for r in range(1, n_row):
            grad += g_buf[step, r]
        x_old = x_ref[0]
        x_new = jnp.minimum(jnp.maximum(x_old + TAU * grad, x_ref[1]), x_ref[2])
        x_ref[0] = x_new
        z_ref[...] = 2.0 * x_new - x_old
        moved = jnp.where(owner == me_row, x_new - x_old, 0.0)
        for k in range(slots):
            pieces[k : k + 1, :] = z_ref[pl.ds(col_of[k], 1), :]
        applied = spread(products(w_n), row_to, row_blocks)
        for c in range(n_col):
            p_send[step, c] = applied[c * dual_rows : (c + 1) * dual_rows]
        to_col(
            lambda other: p_send.at[step, other], p_recv.at[step, me_col],
            p_send_sem.at[step], p_recv_sem.at[step],
        )
        p_recv[step, me_col] = p_send[step, me_col]
        moved_sum = jnp.sum(moved * moved, axis=0, keepdims=True)
        await_bytes(p_recv.at[step, pl.ds(0, n_col - 1)], p_recv_sem.at[step])
        product = p_recv[step, 0]
        for c in range(1, n_col):
            product += p_recv[step, c]
        resid = rhs_own - product
        y_own = y_own + SIGMA * resid
        if step + 1 < ITERS:
            y_buf[step + 1, me_col] = y_own
            to_col(
                lambda other: y_buf.at[step + 1, me_col], y_buf.at[step + 1, me_col],
                y_send_sem.at[step + 1], y_recv_sem.at[step + 1],
            )
        sums.append(jnp.sum(resid * resid, axis=0, keepdims=True))
        sums.append(moved_sum)

    table = jnp.sum(jnp.concatenate(sums, axis=0), axis=1, keepdims=True)
    table = jnp.broadcast_to(table, (2 * ITERS, side))
    at_row = lax.broadcasted_iota(jnp.int32, (2 * ITERS, side), 0)
    at_lane = lax.broadcasted_iota(jnp.int32, (2 * ITERS, side), 1)
    n_buf[me] = jnp.sum(jnp.where(at_row == at_lane, table, 0.0), axis=0, keepdims=True)

    def tell(step):
        other = lax.rem(me + step, total)
        pltpu.make_async_remote_copy(
            src_ref=n_buf.at[me], dst_ref=n_buf.at[me], send_sem=n_send_sem, recv_sem=n_recv_sem,
            device_id=(other // n_row, lax.rem(other, n_row)), device_id_type=MESH,
        ).start()

    each(total, tell)

    x_value = x_ref[0]
    mine = x_value[0:primal_rows]
    for r in range(1, n_row):
        mine = jnp.where(me_row == r, x_value[r * primal_rows : (r + 1) * primal_rows], mine)
    primal_out[...] = mine
    dual_out[...] = y_own

    await_bytes(y_buf.at[0, pl.ds(0, n_col - 1)], y_send_sem.at[0])
    for index in range(3):
        await_bytes(bounds.at[index, pl.ds(0, n_row - 1)], bound_send.at[index])
    for step in range(ITERS):
        if step:
            await_bytes(y_buf.at[step, pl.ds(0, n_col - 1)], y_send_sem.at[step])
        await_bytes(g_buf.at[step, pl.ds(0, n_row - 1)], g_send_sem.at[step])
        await_bytes(p_recv.at[step, pl.ds(0, n_col - 1)], p_send_sem.at[step])

    await_bytes(n_buf.at[pl.ds(0, total - 1)], n_recv_sem)
    norms = jnp.sqrt(jnp.sum(n_buf[...], axis=0))
    wide = jnp.broadcast_to(norms, (8, side))
    at_row = lax.broadcasted_iota(jnp.int32, (8, side), 0)
    at_lane = lax.broadcasted_iota(jnp.int32, (8, side), 1)
    first = jnp.sum(jnp.where(at_lane == 2 * at_row, wide, 0.0), axis=1, keepdims=True)
    second = jnp.sum(jnp.where(at_lane == 2 * at_row + 1, wide, 0.0), axis=1, keepdims=True)
    norms_out[...] = jnp.where(at_lane == 0, first, second)[0:ITERS, 0:2]
    await_bytes(n_buf.at[pl.ds(0, total - 1)], n_send_sem)


def local(blocks, row_index, col_index, counts, rhs, lower, upper, primal_start, dual_start):
    slots, side = blocks.shape[2], blocks.shape[3]
    n_col = lax.axis_size("col")
    n_row = lax.axis_size("row")
    primal_rows = primal_start.shape[0] // side
    dual_rows = dual_start.shape[0] // side
    row_blocks = dual_rows * n_col
    col_blocks = primal_rows * n_row
    hbm = pl.BlockSpec(memory_space=pltpu.HBM)
    smem = pl.BlockSpec(memory_space=pltpu.SMEM)
    vmem = pl.BlockSpec(memory_space=pltpu.VMEM)
    f32 = jnp.float32
    dma = pltpu.SemaphoreType.DMA
    primal, dual, norms = pl.pallas_call(
        functools.partial(kernel, n_col, n_row),
        out_shape=(
            jax.ShapeDtypeStruct((primal_rows, side), f32),
            jax.ShapeDtypeStruct((dual_rows, side), f32),
            jax.ShapeDtypeStruct((ITERS, 2), f32),
        ),
        in_specs=[hbm, smem, smem, smem, hbm, hbm, hbm, hbm, hbm],
        out_specs=(vmem, vmem, vmem),
        scratch_shapes=[
            pltpu.VMEM((slots, side, side), f32),
            pltpu.VMEM((2 * side, slots * side), jnp.bfloat16),
            pltpu.VMEM((2 * side, slots * side), jnp.bfloat16),
            pltpu.VMEM((slots, side), f32),
            pltpu.VMEM((3, n_row, primal_rows, side), f32),
            pltpu.VMEM((dual_rows, side), f32),
            pltpu.VMEM((ITERS, n_col, dual_rows, side), f32),
            pltpu.VMEM((ITERS, n_row, col_blocks, side), f32),
            pltpu.VMEM((ITERS, n_col, dual_rows, side), f32),
            pltpu.VMEM((ITERS, n_col, dual_rows, side), f32),
            pltpu.VMEM((3, col_blocks, side), f32),
            pltpu.VMEM((col_blocks, side), f32),
            pltpu.VMEM((n_col * n_row, 1, side), f32),
            dma, dma((5,)), dma((3,)), dma((3,)), dma((ITERS,)), dma((ITERS,)),
            dma((ITERS,)), dma((ITERS,)), dma((ITERS,)), dma((ITERS,)), dma, dma,
        ],
        compiler_params=pltpu.CompilerParams(collective_id=0, has_side_effects=True),
    )(
        blocks.reshape(slots, side, side),
        row_index.reshape(1, slots),
        col_index.reshape(1, slots),
        counts.reshape(1, 1),
        rhs.reshape(dual_rows, side),
        lower.reshape(primal_rows, side),
        upper.reshape(primal_rows, side),
        primal_start.reshape(primal_rows, side),
        dual_start.reshape(dual_rows, side),
    )
    return primal.reshape(-1), dual.reshape(-1), norms


def solution(mesh):
    in_specs = (
        P("col", "row", None, None, None),
        P("col", "row", None),
        P("col", "row", None),
        P("col", "row"),
        P(("row", "col")),
        P(("col", "row")),
        P(("col", "row")),
        P(("col", "row")),
        P(("row", "col")),
    )
    out_specs = (P(("col", "row")), P(("row", "col")), P())
    return jax.shard_map(local, mesh=mesh, in_specs=in_specs, out_specs=out_specs, check_vma=False)
```

```python
import functools

import jax
import jax.numpy as jnp
from jax import lax
from jax.experimental import pallas as pl
from jax.experimental.pallas import tpu as pltpu
from jax.sharding import PartitionSpec as P

ITERS = 3
TAU = 0.4
SIGMA = 0.4
MESH = pl.DeviceIdType.MESH


def each(count, body):
    if count <= 32:
        for step in range(1, count):
            body(step)
    else:
        lax.fori_loop(1, count, lambda step, carry: (body(step), carry)[1], 0)


def split(value):
    high = value.astype(jnp.bfloat16).astype(jnp.float32)
    return high, value - high


def left_operand(value):
    high, low = split(value)
    first = jnp.concatenate([high, low], axis=0)
    second = jnp.concatenate([high, jnp.zeros_like(low)], axis=0)
    return jnp.concatenate([first, second], axis=1).astype(jnp.bfloat16)


def kernel(
    n_col, n_row,
    blocks, rows, cols, counts, rhs, lower, upper, primal, dual,
    primal_out, dual_out, norms_out,
    tiles, w_t, w_n, pieces,
    bounds, own_vec, y_buf, g_buf, p_send, p_recv, x_ref, z_ref, n_buf,
    load_sem, own_sem, bound_send, bound_recv, y_send_sem, y_recv_sem,
    g_send_sem, g_recv_sem, p_send_sem, p_recv_sem, n_send_sem, n_recv_sem,
):
    slots, side = tiles.shape[0], tiles.shape[1]
    dual_rows = dual.shape[0]
    primal_rows = primal.shape[0]
    row_blocks = dual_rows * n_col
    col_blocks = primal_rows * n_row
    total = n_col * n_row
    me_col = lax.axis_index("col")
    me_row = lax.axis_index("row")
    me = me_col * n_row + me_row

    load = pltpu.make_async_copy(blocks, tiles, load_sem)
    load.start()
    own_copies = []
    for index, source in enumerate((primal, lower, upper)):
        copy = pltpu.make_async_copy(source, bounds.at[index, me_row], own_sem.at[index])
        copy.start()
        own_copies.append(copy)
    for index, (source, target) in enumerate(((dual, y_buf.at[0, me_col]), (rhs, own_vec))):
        copy = pltpu.make_async_copy(source, target, own_sem.at[3 + index])
        copy.start()
        own_copies.append(copy)

    barrier = pltpu.get_barrier_semaphore()

    def greet_col(step):
        other = (lax.rem(me_col + step, n_col), me_row)
        pl.semaphore_signal(barrier, inc=1, device_id=other, device_id_type=MESH)

    def greet_row(step):
        other = (me_col, lax.rem(me_row + step, n_row))
        pl.semaphore_signal(barrier, inc=1, device_id=other, device_id_type=MESH)

    each(n_col, greet_col)
    each(n_row, greet_row)
    pl.semaphore_wait(barrier, n_col + n_row - 2)

    def to_col(source, target, send, recv):
        def body(step):
            other = lax.rem(me_col + step, n_col)
            pltpu.make_async_remote_copy(
                src_ref=source(other), dst_ref=target, send_sem=send, recv_sem=recv,
                device_id=(other, me_row), device_id_type=MESH,
            ).start()

        each(n_col, body)

    def to_row(source, target, send, recv):
        def body(step):
            other = lax.rem(me_row + step, n_row)
            pltpu.make_async_remote_copy(
                src_ref=source, dst_ref=target, send_sem=send, recv_sem=recv,
                device_id=(me_col, other), device_id_type=MESH,
            ).start()

        each(n_row, body)

    def await_bytes(ref, sem):
        pltpu.make_async_copy(ref, ref, sem).wait()

    own_copies[3].wait()
    to_col(lambda other: y_buf.at[0, me_col], y_buf.at[0, me_col], y_send_sem.at[0], y_recv_sem.at[0])
    for index, source in enumerate((primal, lower, upper)):
        own_copies[index].wait()
        to_row(bounds.at[index, me_row], bounds.at[index, me_row], bound_send.at[index], bound_recv.at[index])

    load.wait()
    for k in range(slots):
        tile = tiles[k]
        high, low = split(tile)
        w_t[0:side, k * side : (k + 1) * side] = high.astype(jnp.bfloat16)
        w_t[side : 2 * side, k * side : (k + 1) * side] = low.astype(jnp.bfloat16)
        high, low = split(tile.T)
        w_n[0:side, k * side : (k + 1) * side] = high.astype(jnp.bfloat16)
        w_n[side : 2 * side, k * side : (k + 1) * side] = low.astype(jnp.bfloat16)

    live = counts[0, 0]
    row_of = [rows[0, k] for k in range(slots)]
    col_of = [cols[0, k] for k in range(slots)]
    row_to = [jnp.where(k < live, row_of[k], -1) for k in range(slots)]
    col_to = [jnp.where(k < live, col_of[k], -1) for k in range(slots)]

    def products(weights):
        outs = []
        group = 8
        for base in range(0, slots, group):
            end = min(slots, base + group)
            left = left_operand(pieces[base:end, :])
            result = jnp.dot(
                left, weights[:, base * side : end * side], preferred_element_type=jnp.float32
            )
            for k in range(end - base):
                at = slice(k * side, (k + 1) * side)
                low = end - base + k
                outs.append(result[k : k + 1, at] + result[low : low + 1, at])
        return outs

    def spread(outs, targets, count):
        places = lax.broadcasted_iota(jnp.int32, (count, side), 0)
        total_value = jnp.zeros((count, side), jnp.float32)
        for k in range(slots):
            total_value += jnp.where(places == targets[k], outs[k], 0.0)
        return total_value

    own_copies[4].wait()
    for index in range(3):
        await_bytes(bounds.at[index, pl.ds(0, n_row - 1)], bound_recv.at[index])
    groups = []
    for index in range(3):
        groups.append(jnp.concatenate([bounds[index, r] for r in range(n_row)], axis=0))
    x_value, low_value, high_value = groups
    x_ref[0] = x_value
    x_ref[1] = low_value
    x_ref[2] = high_value
    y_own = y_buf[0, me_col]
    rhs_own = own_vec[...]
    owner = lax.broadcasted_iota(jnp.int32, (col_blocks, side), 0) // primal_rows
    sums = []

    for step in range(ITERS):
        await_bytes(y_buf.at[step, pl.ds(0, n_col - 1)], y_recv_sem.at[step])
        for k in range(slots):
            r = row_of[k]
            pieces[k : k + 1, :] = y_buf[step, r // dual_rows, pl.ds(lax.rem(r, dual_rows), 1), :]
        partial = spread(products(w_t), col_to, col_blocks)
        g_buf[step, me_row] = partial
        to_row(
            g_buf.at[step, me_row], g_buf.at[step, me_row], g_send_sem.at[step], g_recv_sem.at[step]
        )
        await_bytes(g_buf.at[step, pl.ds(0, n_row - 1)], g_recv_sem.at[step])
        grad = g_buf[step, 0]
        for r in range(1, n_row):
            grad += g_buf[step, r]
        x_old = x_ref[0]
        x_new = jnp.minimum(jnp.maximum(x_old + TAU * grad, x_ref[1]), x_ref[2])
        x_ref[0] = x_new
        z_ref[...] = 2.0 * x_new - x_old
        moved = jnp.where(owner == me_row, x_new - x_old, 0.0)
        for k in range(slots):
            pieces[k : k + 1, :] = z_ref[pl.ds(col_of[k], 1), :]
        applied = spread(products(w_n), row_to, row_blocks)
        for c in range(n_col):
            p_send[step, c] = applied[c * dual_rows : (c + 1) * dual_rows]
        to_col(
            lambda other: p_send.at[step, other], p_recv.at[step, me_col],
            p_send_sem.at[step], p_recv_sem.at[step],
        )
        p_recv[step, me_col] = p_send[step, me_col]
        moved_sum = jnp.sum(moved * moved, axis=0, keepdims=True)
        await_bytes(p_recv.at[step, pl.ds(0, n_col - 1)], p_recv_sem.at[step])
        product = p_recv[step, 0]
        for c in range(1, n_col):
            product += p_recv[step, c]
        resid = rhs_own - product
        y_own = y_own + SIGMA * resid
        if step + 1 < ITERS:
            y_buf[step + 1, me_col] = y_own
            to_col(
                lambda other: y_buf.at[step + 1, me_col], y_buf.at[step + 1, me_col],
                y_send_sem.at[step + 1], y_recv_sem.at[step + 1],
            )
        sums.append(jnp.sum(resid * resid, axis=0, keepdims=True))
        sums.append(moved_sum)

    table = jnp.sum(jnp.concatenate(sums, axis=0), axis=1, keepdims=True)
    table = jnp.broadcast_to(table, (2 * ITERS, side))
    at_row = lax.broadcasted_iota(jnp.int32, (2 * ITERS, side), 0)
    at_lane = lax.broadcasted_iota(jnp.int32, (2 * ITERS, side), 1)
    n_buf[me] = jnp.sum(jnp.where(at_row == at_lane, table, 0.0), axis=0, keepdims=True)

    def tell(step):
        other = lax.rem(me + step, total)
        pltpu.make_async_remote_copy(
            src_ref=n_buf.at[me], dst_ref=n_buf.at[me], send_sem=n_send_sem, recv_sem=n_recv_sem,
            device_id=(other // n_row, lax.rem(other, n_row)), device_id_type=MESH,
        ).start()

    each(total, tell)

    x_value = x_ref[0]
    mine = x_value[0:primal_rows]
    for r in range(1, n_row):
        mine = jnp.where(me_row == r, x_value[r * primal_rows : (r + 1) * primal_rows], mine)
    primal_out[...] = mine
    dual_out[...] = y_own

    await_bytes(y_buf.at[0, pl.ds(0, n_col - 1)], y_send_sem.at[0])
    for index in range(3):
        await_bytes(bounds.at[index, pl.ds(0, n_row - 1)], bound_send.at[index])
    for step in range(ITERS):
        if step:
            await_bytes(y_buf.at[step, pl.ds(0, n_col - 1)], y_send_sem.at[step])
        await_bytes(g_buf.at[step, pl.ds(0, n_row - 1)], g_send_sem.at[step])
        await_bytes(p_recv.at[step, pl.ds(0, n_col - 1)], p_send_sem.at[step])

    await_bytes(n_buf.at[pl.ds(0, total - 1)], n_recv_sem)
    norms = jnp.sqrt(jnp.sum(n_buf[...], axis=0))
    wide = jnp.broadcast_to(norms, (8, side))
    at_row = lax.broadcasted_iota(jnp.int32, (8, side), 0)
    at_lane = lax.broadcasted_iota(jnp.int32, (8, side), 1)
    outputs = jnp.zeros((8, side), jnp.float32)
    for k in range(ITERS):
        chosen = jnp.where(at_lane == 2 * k + at_row, wide, 0.0)
        outputs = jnp.where(at_lane == k, jnp.sum(chosen, axis=1, keepdims=True), outputs)
    norms_out[...] = outputs
    await_bytes(n_buf.at[pl.ds(0, total - 1)], n_send_sem)


def finish_kernel(primal, dual, norms, primal_out, dual_out, norms_out):
    primal_out[...] = primal[...]
    dual_out[...] = dual[...]
    norms_out[...] = norms[0:2, 0:ITERS]


def finish(primal, dual, norms):
    vmem = pl.BlockSpec(memory_space=pltpu.VMEM)
    primal, dual, norms = pl.pallas_call(
        finish_kernel,
        out_shape=(
            jax.ShapeDtypeStruct(primal.shape, jnp.float32),
            jax.ShapeDtypeStruct(dual.shape, jnp.float32),
            jax.ShapeDtypeStruct((2, ITERS), jnp.float32),
        ),
        in_specs=[vmem] * 3,
        out_specs=(vmem,) * 3,
    )(primal, dual, norms)
    return primal.reshape(-1), dual.reshape(-1), norms.T


def local(blocks, row_index, col_index, counts, rhs, lower, upper, primal_start, dual_start):
    slots, side = blocks.shape[2], blocks.shape[3]
    n_col = lax.axis_size("col")
    n_row = lax.axis_size("row")
    primal_rows = primal_start.shape[0] // side
    dual_rows = dual_start.shape[0] // side
    row_blocks = dual_rows * n_col
    col_blocks = primal_rows * n_row
    hbm = pl.BlockSpec(memory_space=pltpu.HBM)
    smem = pl.BlockSpec(memory_space=pltpu.SMEM)
    vmem = pl.BlockSpec(memory_space=pltpu.VMEM)
    f32 = jnp.float32
    dma = pltpu.SemaphoreType.DMA
    primal, dual, norms = pl.pallas_call(
        functools.partial(kernel, n_col, n_row),
        out_shape=(
            jax.ShapeDtypeStruct((primal_rows, side), f32),
            jax.ShapeDtypeStruct((dual_rows, side), f32),
            jax.ShapeDtypeStruct((8, side), f32),
        ),
        in_specs=[hbm, smem, smem, smem, hbm, hbm, hbm, hbm, hbm],
        out_specs=(vmem, vmem, vmem),
        scratch_shapes=[
            pltpu.VMEM((slots, side, side), f32),
            pltpu.VMEM((2 * side, slots * side), jnp.bfloat16),
            pltpu.VMEM((2 * side, slots * side), jnp.bfloat16),
            pltpu.VMEM((slots, side), f32),
            pltpu.VMEM((3, n_row, primal_rows, side), f32),
            pltpu.VMEM((dual_rows, side), f32),
            pltpu.VMEM((ITERS, n_col, dual_rows, side), f32),
            pltpu.VMEM((ITERS, n_row, col_blocks, side), f32),
            pltpu.VMEM((ITERS, n_col, dual_rows, side), f32),
            pltpu.VMEM((ITERS, n_col, dual_rows, side), f32),
            pltpu.VMEM((3, col_blocks, side), f32),
            pltpu.VMEM((col_blocks, side), f32),
            pltpu.VMEM((n_col * n_row, 1, side), f32),
            dma, dma((5,)), dma((3,)), dma((3,)), dma((ITERS,)), dma((ITERS,)),
            dma((ITERS,)), dma((ITERS,)), dma((ITERS,)), dma((ITERS,)), dma, dma,
        ],
        compiler_params=pltpu.CompilerParams(collective_id=0, has_side_effects=True),
    )(
        blocks.reshape(slots, side, side),
        row_index.reshape(1, slots),
        col_index.reshape(1, slots),
        counts.reshape(1, 1),
        rhs.reshape(dual_rows, side),
        lower.reshape(primal_rows, side),
        upper.reshape(primal_rows, side),
        primal_start.reshape(primal_rows, side),
        dual_start.reshape(dual_rows, side),
    )
    return finish(primal, dual, norms)


def solution(mesh):
    in_specs = (
        P("col", "row", None, None, None),
        P("col", "row", None),
        P("col", "row", None),
        P("col", "row"),
        P(("row", "col")),
        P(("col", "row")),
        P(("col", "row")),
        P(("col", "row")),
        P(("row", "col")),
    )
    out_specs = (P(("col", "row")), P(("row", "col")), P())
    return jax.shard_map(local, mesh=mesh, in_specs=in_specs, out_specs=out_specs, check_vma=False)
```
